512 devices in a mesh: groups: 2 (over y), expert: 32 (over z, core), mp: 8 (over x).
Axes of the slice: x: 8, y: 2, z: 16, core: 2. Of those that a mesh axis runs over, the one named last changes fastest.
The devices are a block of a 8x16x16 slice.
Arguments:
- tokens: bfloat16 [49152, 1024], P(('groups', 'expert'), 'mp'), parts along dimension 0, may hold values from -60 to 60
- gain: float32 [1024], replicated, may hold values from 0.1 to 1.9
- w_res_in: bfloat16 [1024, 4096], P(None, 'mp'), may hold values from -0.1875 to 0.1875
- w_res_out: bfloat16 [4096, 1024], P('mp'), may hold values from -0.09375 to 0.09375
- w_exp_in: bfloat16 [32, 1024, 4096], P('expert', None, 'mp'), may hold values from -0.1875 to 0.1875
- w_exp_out: bfloat16 [32, 4096, 1024], P('expert', 'mp'), may hold values from -0.09375 to 0.09375
- expert_of: int32 [49152], P(('groups', 'expert')), parts along dimension 0, may hold values from 0 to 31
- slot_of: int32 [49152], P(('groups', 'expert')), parts along dimension 0, may hold values from -1 to 29, as said below
- gate_prob: float32 [49152], P(('groups', 'expert')), parts along dimension 0, may hold values from 0.2 to 1
Outputs:
- layer_out: bfloat16 [49152, 1024], P(('groups', 'expert'), 'mp'), parts along dimension 0
The draws below stay inside these ranges and needn't reach their ends.
There are 2 independent parts, one for each index of `groups`. The reference program is written for one: setup_inputs(seed, part) draws one part's arguments, and reference() takes and returns one part's arrays. A program takes and returns all parts, laid end to end along the dimension named above; an argument that names none is the same for every part. Nothing has to cross between parts.
Inputs may be any that keep to these rules, and one draw needn't show every extreme that they name: slot_of[t] is the number of earlier tokens of t's aligned block of 768 tokens with the same expert_of, or -1 where that number is 30 or more. In every draw one expert has more than 30 tokens in every aligned block.
All inputs are finite; a program needn't handle non-finite values.
Results may differ from the reference program's by a relative error of at most 0.014.
Values may be sent and summed in bfloat16 or wider, within the bound.
No kernel may reach another device: no remote copies, remote signals or barrier semaphores. Data moves between devices by JAX's collectives and lax.ppermute only.
A program may use at most 64 MiB of HBM per device.

```python
import math
import jax
import jax.numpy as jnp
from jax import lax

D = 1024
FE = 4096
FR = 4096
TOK_DEV = 768
EXPERTS = 32
TOKENS = 24576
CAP = 30
N_EXPERT = 32
N_MP = 8


def draw_tokens(key, part):
    mixed = jax.random.fold_in(key, 11)
    key_base, key_rows, key_cols = jax.random.split(mixed, 3)
    base = jnp.clip(jax.random.normal(key_base, (TOKENS, D), jnp.float32), -5.5, 5.5)
    row_scale = jnp.exp(jax.random.uniform(key_rows, (TOKENS, 1), jnp.float32) * math.log(10.0))
    col_scale = jnp.exp(jax.random.uniform(key_cols, (1, D), jnp.float32) * math.log(10.0))
    return (base * row_scale * col_scale / 10.0).astype(jnp.bfloat16)


def shuffle(subkey):
    return jax.random.permutation(subkey, TOK_DEV)


def routing_pair(key):
    mixed = jax.random.fold_in(key, 5)
    key_base, key_hot, key_perm = jax.random.split(mixed, 3)
    blocks = TOKENS // TOK_DEV
    base = jax.random.randint(key_base, (blocks, TOK_DEV), 0, EXPERTS)
    hottest = jax.random.randint(key_hot, (1, 1), 0, EXPERTS)
    order = jax.vmap(shuffle)(jax.random.split(key_perm, blocks))
    chosen = order < CAP + 2
    expert_ids = jnp.where(chosen, hottest, base).astype(jnp.int32)
    same = expert_ids[:, :, None] == expert_ids[:, None, :]
    index = jnp.arange(TOK_DEV, dtype=jnp.int32)
    earlier = index[None, :] < index[:, None]
    rank = jnp.sum(jnp.logical_and(same, earlier[None]).astype(jnp.int32), axis=2)
    slots = jnp.where(rank < CAP, rank, -1).astype(jnp.int32)
    return (expert_ids.reshape(TOKENS), slots.reshape(TOKENS))


def draw_expert_of(key, part):
    return routing_pair(key)[0]


def draw_slot_of(key, part):
    return routing_pair(key)[1]


def level_of(own_key, extent, shards, low, largest):
    loudness = 1.0
    for axis_at, parts in shards:
        heights = jax.random.uniform(jax.random.fold_in(jax.random.fold_in(own_key, 6), axis_at), (parts,), jnp.float32, low / len(shards), largest / len(shards))
        loudness = loudness * jnp.repeat(jnp.exp(heights), extent[axis_at] // parts).reshape((-1,) + (1,) * (len(extent) - 1 - axis_at))
    return loudness


def gaussian(stream_key, dims, deviation, most, shards=(), kind=jnp.bfloat16):
    result = jax.random.normal(stream_key, dims, jnp.float32) * deviation
    if len(shards) > 0:
        result = level_of(stream_key, dims, shards, -0.22, 0.18) * result
    return jnp.clip(result, min=-most, max=most).astype(kind)


def setup_inputs(seed: int = 0, part: int = 0) -> dict:
    arg_keys = jax.random.split(jax.random.key(seed), 10)
    part_keys = jax.random.split(jax.random.fold_in(arg_keys[9], part), 10)
    return {
        "tokens": draw_tokens(jax.random.fold_in(jax.random.fold_in(arg_keys[9], part), 71), part),
        "gain": jnp.clip(1.0 + 0.18 * jax.random.normal(arg_keys[1], (D,), jnp.float32), 0.1, 1.9),
        "w_res_in": gaussian(arg_keys[2], (D, FR), D ** -0.5, 0.1875, ((1, 8),)),
        "w_res_out": gaussian(arg_keys[3], (FR, D), FR ** -0.5, 0.09375, ((0, 8),)),
        "w_exp_in": gaussian(arg_keys[4], (EXPERTS, D, FE), D ** -0.5, 0.1875, ((0, 32), (2, 8))),
        "w_exp_out": gaussian(arg_keys[5], (EXPERTS, FE, D), FE ** -0.5, 0.09375, ((0, 32), (1, 8))),
        "expert_of": draw_expert_of(jax.random.fold_in(jax.random.fold_in(arg_keys[9], part), 71), part),
        "slot_of": draw_slot_of(jax.random.fold_in(jax.random.fold_in(arg_keys[9], part), 71), part),
        "gate_prob": jnp.clip(jnp.exp(math.log(1.0) - 1.609438 * jax.random.uniform(part_keys[8], (TOKENS,), jnp.float32) ** level_of(part_keys[8], (TOKENS,), ((0, 32),), -0.2, 0.2)), 0.2, 1.0),
    }


def rms_rows(tokens, gain):
    values = tokens.astype(jnp.float32)
    inverse = lax.rsqrt(lax.optimization_barrier(jnp.mean(values * values, axis=-1, keepdims=True)) + 1e-05)
    return (values * inverse * gain.astype(jnp.float32)).astype(jnp.bfloat16)

def block_sums(hidden, w_out):
    width = hidden.shape[1] // N_MP
    total = jnp.zeros((hidden.shape[0], w_out.shape[1]), jnp.float32)
    for block in range(N_MP):
        part = jnp.dot(hidden[:, block * width:(block + 1) * width], w_out[block * width:(block + 1) * width], preferred_element_type=jnp.float32)
        total = total + part.astype(jnp.bfloat16).astype(jnp.float32)
    return total

def reference(tokens, gain, w_res_in, w_res_out, w_exp_in, w_exp_out, expert_of, slot_of, gate_prob):
    normed = rms_rows(tokens, gain)
    res_hidden = jax.nn.gelu(jnp.dot(normed, w_res_in, preferred_element_type=jnp.float32)).astype(jnp.bfloat16)
    res_sum = block_sums(res_hidden, w_res_out)
    blocks = N_EXPERT
    position = jnp.arange(TOKENS, dtype=jnp.int32)
    block_of = position // TOK_DEV
    slots_all = EXPERTS * blocks * CAP
    destination = jnp.where(slot_of >= 0, expert_of * (blocks * CAP) + block_of * CAP + slot_of, slots_all).astype(jnp.int32)
    buffer = jnp.zeros((slots_all + 1, D), jnp.bfloat16).at[destination].set(normed)
    expert_in = buffer[:slots_all].reshape(EXPERTS, blocks * CAP, D)

    def one_expert(item):
        rows, w_in, w_out = item
        hidden = jax.nn.gelu(jnp.dot(rows, w_in, preferred_element_type=jnp.float32)).astype(jnp.bfloat16)
        return block_sums(hidden, w_out).astype(jnp.bfloat16)
    expert_out = lax.map(one_expert, (expert_in, w_exp_in, w_exp_out))
    flat_rows = jnp.concatenate([expert_out.reshape(slots_all, D), jnp.zeros((1, D), jnp.bfloat16)], axis=0)
    moe_value = flat_rows[destination].astype(jnp.float32)
    return (res_sum + gate_prob[:, None] * moe_value).astype(jnp.bfloat16)
```

```python
import functools

import jax
import jax.numpy as jnp
from jax import lax
from jax.experimental import pallas as pl
from jax.experimental.pallas import tpu as pltpu
from jax.sharding import PartitionSpec as P


def from_everyone(shard, axis):
    devices = lax.axis_size(axis)
    return lax.all_to_all(
        jnp.broadcast_to(shard[None], (devices, *shard.shape)), axis, 0, 0, tiled=True
    )


def ffn_body(rows_ref, gain_ref, w_in_ref, w_out_ref, *rest):
    out_ref = rest[-1]
    parts = rows_ref.shape[0]
    width = rows_ref.shape[2]
    values = jnp.concatenate([rows_ref[k] for k in range(parts)], axis=1).astype(jnp.float32)
    inverse = lax.rsqrt(jnp.mean(values * values, axis=1, keepdims=True) + 1e-05)
    normed = (values * inverse * gain_ref[...]).astype(jnp.bfloat16)
    preact = jnp.dot(normed, w_in_ref[...], preferred_element_type=jnp.float32)
    hidden = jax.nn.gelu(preact, approximate=True).astype(jnp.bfloat16)
    sums = jnp.dot(hidden, w_out_ref[...], preferred_element_type=jnp.float32).astype(jnp.bfloat16)
    for k in range(parts):
        out_ref[k] = sums[:, k * width : (k + 1) * width]


def ffn(rows, gain, w_in, w_out, block, total, offset, into=None):
    parts, count, width = rows.shape
    model = parts * width
    first = offset // block
    in_specs = [
        pl.BlockSpec((parts, block, width), lambda i: (0, i, 0)),
        pl.BlockSpec((1, model), lambda i: (0, 0)),
        pl.BlockSpec(w_in.shape, lambda i: (0, 0)),
        pl.BlockSpec(w_out.shape, lambda i: (0, 0)),
    ]
    operands = [rows, gain.reshape(1, model), w_in, w_out]
    aliases = {}
    if into is not None:
        in_specs.append(pl.BlockSpec(memory_space=pl.ANY))
        operands.append(into)
        aliases = {4: 0}
    return pl.pallas_call(
        ffn_body,
        grid=(count // block,),
        in_specs=in_specs,
        out_specs=pl.BlockSpec((parts, block, width), lambda i: (0, first + i, 0)),
        out_shape=jax.ShapeDtypeStruct((parts, total, width), jnp.bfloat16),
        input_output_aliases=aliases,
        compiler_params=pltpu.CompilerParams(
            dimension_semantics=("arbitrary",), vmem_limit_bytes=40 * 1024 * 1024
        ),
        cost_estimate=pl.CostEstimate(
            flops=4 * count * model * w_in.shape[1],
            transcendentals=count * w_in.shape[1],
            bytes_accessed=4 * count * model + 4 * model * w_in.shape[1],
        ),
        name="ffn",
    )(*operands)


def per_device(
    tokens, gain, w_res_in, w_res_out, w_exp_in, w_exp_out, expert_of, slot_of, gate_prob
):
    row_count, feat_width = tokens.shape
    experts = lax.axis_size("expert")
    capacity = max(2, 5 * row_count // (4 * experts))
    slots = experts * capacity
    half = slots // 2
    slot_id = jnp.where(slot_of >= 0, expert_of * capacity + slot_of, -1)
    slot_index = jnp.arange(slots, dtype=jnp.int32)
    send_table = (slot_index[:, None] == slot_id[None, :]).astype(jnp.bfloat16)
    take_table = (slot_id[:, None] == slot_index[None, :]).astype(jnp.bfloat16)
    res_rows = lax.all_gather(tokens, "mp", axis=0)
    outgoing = jnp.dot(send_table, tokens, preferred_element_type=jnp.float32).astype(jnp.bfloat16)
    incoming = lax.all_to_all(
        outgoing.reshape(experts, capacity, feat_width),
        "expert",
        split_axis=0,
        concat_axis=0,
        tiled=True,
    ).reshape(slots, feat_width)
    rows_b = from_everyone(incoming[half:], "mp")
    rows_a = lax.all_gather(incoming[:half], "mp", axis=0)
    total = slots + row_count
    sums = ffn(res_rows, gain, w_res_in, w_res_out, row_count // 4, total, slots)
    sums = ffn(rows_a, gain, w_exp_in[0], w_exp_out[0], half // 2, total, 0, sums)
    sums = ffn(rows_b, gain, w_exp_in[0], w_exp_out[0], half // 2, total, half, sums)
    summed = lax.psum_scatter(sums, "mp", scatter_dimension=0, tiled=False)
    returned = lax.all_to_all(
        summed[:slots].reshape(experts, capacity, feat_width),
        "expert",
        split_axis=0,
        concat_axis=0,
        tiled=True,
    )
    moe_value = jnp.dot(
        take_table, returned.reshape(slots, feat_width), preferred_element_type=jnp.float32
    )
    res_sum = summed[slots:].astype(jnp.float32)
    return (res_sum + gate_prob[:, None] * moe_value).astype(jnp.bfloat16)


def solution(mesh):
    return jax.shard_map(
        per_device,
        mesh=mesh,
        in_specs=(
            P(("groups", "expert"), "mp"),
            P(),
            P(None, "mp"),
            P("mp", None),
            P("expert", None, "mp"),
            P("expert", "mp", None),
            P(("groups", "expert")),
            P(("groups", "expert")),
            P(("groups", "expert")),
        ),
        out_specs=P(("groups", "expert"), "mp"),
        check_vma=False,
    )
```

```python
import functools

import jax
import jax.numpy as jnp
from jax import lax
from jax.experimental import pallas as pl
from jax.experimental.pallas import tpu as pltpu
from jax.sharding import PartitionSpec as P

RING = 8


def shift(value, step, axis="mp"):
    ring = lax.axis_size(axis)
    return lax.ppermute(value, axis, [(i, (i + step) % ring) for i in range(ring)])


def gather_far(own):
    return shift(own, 3), shift(own, -3)


def gather_near(own, below, above):
    half = own.shape[0] // 2
    from_left = shift(jnp.concatenate([own, above, below[:half]], axis=0), 1)
    from_right = shift(jnp.concatenate([own, below, above[half:]], axis=0), -1)
    return from_left, from_right


def ffn_body(
    me_ref,
    own_ref,
    below_ref,
    above_ref,
    left_ref,
    right_ref,
    gain_ref,
    w_in_ref,
    w_out_ref,
    to_right_ref,
    to_left_ref,
    keep_ref,
    rows_ref,
    sums_ref,
    *,
    block,
):
    me = me_ref[0]
    count, width = own_ref.shape
    half = count // 2
    place = [lax.rem(me + step, RING) for step in range(RING)]
    for start in range(0, count, block):
        at = pl.ds(start, block)
        rows_ref[place[0], at] = own_ref[at]
        rows_ref[place[1], at] = right_ref[at]
        rows_ref[place[7], at] = left_ref[at]
        rows_ref[place[3], at] = above_ref[at]
        rows_ref[place[5], at] = below_ref[at]
        rows_ref[place[2], at] = left_ref[pl.ds(count + start, block)]
        rows_ref[place[6], at] = right_ref[pl.ds(count + start, block)]
        if start < half:
            rows_ref[place[4], at] = left_ref[pl.ds(2 * count + start, block)]
        else:
            rows_ref[place[4], at] = right_ref[pl.ds(2 * count + start - half, block)]
        values = jnp.concatenate([rows_ref[k, at] for k in range(RING)], axis=1)
        values = values.astype(jnp.float32)
        inverse = lax.rsqrt(jnp.mean(values * values, axis=1, keepdims=True) + 1e-05)
        normed = (values * inverse * gain_ref[...]).astype(jnp.bfloat16)
        preact = jnp.dot(normed, w_in_ref[...], preferred_element_type=jnp.float32)
        hidden = jax.nn.gelu(preact, approximate=True).astype(jnp.bfloat16)
        sums = jnp.dot(hidden, w_out_ref[...], preferred_element_type=jnp.float32)
        sums = sums.astype(jnp.bfloat16)
        for k in range(RING):
            sums_ref[k, at] = sums[:, k * width : (k + 1) * width]
        to_right_ref[at] = sums_ref[place[1], at]
        to_right_ref[pl.ds(count + start, block)] = sums_ref[place[6], at]
        to_left_ref[at] = sums_ref[place[7], at]
        to_left_ref[pl.ds(count + start, block)] = sums_ref[place[2], at]
        if start < half:
            to_right_ref[pl.ds(2 * count + start, block)] = sums_ref[place[4], at]
        else:
            to_left_ref[pl.ds(2 * count + start - half, block)] = sums_ref[place[4], at]
        keep_ref[0, at] = sums_ref[place[0], at]
        keep_ref[1, at] = sums_ref[place[3], at]
        keep_ref[2, at] = sums_ref[place[5], at]


def ffn(me, own, below, above, left, right, gain, w_in, w_out, name):
    count, width = own.shape
    model = RING * width
    vmem = pl.BlockSpec(memory_space=pltpu.VMEM)
    edge = jax.ShapeDtypeStruct((5 * count // 2, width), jnp.bfloat16)
    return pl.pallas_call(
        functools.partial(ffn_body, block=count // 4),
        in_specs=[pl.BlockSpec(memory_space=pltpu.SMEM)] + [vmem] * 8,
        out_specs=[vmem] * 3,
        out_shape=[edge, edge, jax.ShapeDtypeStruct((3, count, width), jnp.bfloat16)],
        scratch_shapes=[
            pltpu.VMEM((RING, count, width), jnp.bfloat16),
            pltpu.VMEM((RING, count, width), jnp.bfloat16),
        ],
        compiler_params=pltpu.CompilerParams(vmem_limit_bytes=32 * 1024 * 1024),
        cost_estimate=pl.CostEstimate(
            flops=4 * count * model * w_in.shape[1],
            transcendentals=count * w_in.shape[1],
            bytes_accessed=4 * count * model + 4 * model * w_in.shape[1],
        ),
        name=name,
    )(me, own, below, above, left, right, gain.reshape(1, model), w_in, w_out)


def scatter_near(to_right, to_left):
    return shift(to_right, 1), shift(to_left, -1)


def scatter_far(keep, from_left, from_right):
    count = keep.shape[1]
    half = count // 2
    keep = keep.astype(jnp.float32)
    from_left = from_left.astype(jnp.float32)
    from_right = from_right.astype(jnp.float32)
    own = keep[0] + from_left[:count] + from_right[:count]
    above = keep[1] + from_right[count : 2 * count]
    above = jnp.concatenate([above[:half] + from_left[2 * count :], above[half:]], axis=0)
    below = keep[2] + from_left[count : 2 * count]
    below = jnp.concatenate([below[:half], below[half:] + from_right[2 * count :]], axis=0)
    first = shift(above.astype(jnp.bfloat16), 3)
    second = shift(below.astype(jnp.bfloat16), -3)
    return own, first, second


def per_device(
    tokens, gain, w_res_in, w_res_out, w_exp_in, w_exp_out, expert_of, slot_of, gate_prob
):
    row_count, feat_width = tokens.shape
    experts = lax.axis_size("expert")
    capacity = max(2, 5 * row_count // (4 * experts))
    slots = experts * capacity
    me = lax.axis_index("mp").astype(jnp.int32).reshape(1)
    slot_id = jnp.where(slot_of >= 0, expert_of * capacity + slot_of, -1)
    slot_index = jnp.arange(slots, dtype=jnp.int32)
    send_table = (slot_index[:, None] == slot_id[None, :]).astype(jnp.bfloat16)
    take_table = (slot_id[:, None] == slot_index[None, :]).astype(jnp.bfloat16)
    outgoing = jnp.dot(send_table, tokens, preferred_element_type=jnp.float32).astype(jnp.bfloat16)
    incoming = lax.all_to_all(
        outgoing.reshape(experts, capacity, feat_width),
        "expert",
        split_axis=0,
        concat_axis=0,
        tiled=True,
    ).reshape(slots, feat_width)
    with jax.named_scope("res_gather"):
        res_below, res_above = gather_far(tokens)
        res_left, res_right = gather_near(tokens, res_below, res_above)
    with jax.named_scope("exp_gather"):
        exp_below, exp_above = gather_far(incoming)
        exp_left, exp_right = gather_near(incoming, exp_below, exp_above)
    res_to_right, res_to_left, res_keep = ffn(
        me, tokens, res_below, res_above, res_left, res_right, gain, w_res_in, w_res_out, "res_ffn"
    )
    exp_to_right, exp_to_left, exp_keep = ffn(
        me,
        incoming,
        exp_below,
        exp_above,
        exp_left,
        exp_right,
        gain,
        w_exp_in[0],
        w_exp_out[0],
        "exp_ffn",
    )
    with jax.named_scope("exp_scatter"):
        exp_own, exp_first, exp_second = scatter_far(
            exp_keep, *scatter_near(exp_to_right, exp_to_left)
        )
        summed = exp_own + exp_first.astype(jnp.float32) + exp_second.astype(jnp.float32)
        summed = summed.astype(jnp.bfloat16)
    returned = lax.all_to_all(
        summed.reshape(experts, capacity, feat_width),
        "expert",
        split_axis=0,
        concat_axis=0,
        tiled=True,
    )
    with jax.named_scope("res_scatter"):
        res_own, res_first, res_second = scatter_far(
            res_keep, *scatter_near(res_to_right, res_to_left)
        )
        res_sum = res_own + res_first.astype(jnp.float32) + res_second.astype(jnp.float32)
    moe_value = jnp.dot(
        take_table, returned.reshape(slots, feat_width), preferred_element_type=jnp.float32
    )
    return (res_sum + gate_prob[:, None] * moe_value).astype(jnp.bfloat16)


def solution(mesh):
    return jax.shard_map(
        per_device,
        mesh=mesh,
        in_specs=(
            P(("groups", "expert"), "mp"),
            P(),
            P(None, "mp"),
            P("mp", None),
            P("expert", None, "mp"),
            P("expert", "mp", None),
            P(("groups", "expert")),
            P(("groups", "expert")),
            P(("groups", "expert")),
        ),
        out_specs=P(("groups", "expert"), "mp"),
        check_vma=False,
    )
```

```python
import functools

import jax
import jax.numpy as jnp
from jax import lax
from jax.experimental import pallas as pl
from jax.experimental.pallas import tpu as pltpu
from jax.sharding import PartitionSpec as P


RING = 8


def shift(value, step, axis="mp"):
    ring = lax.axis_size(axis)
    return lax.ppermute(value, axis, [(i, (i + step) % ring) for i in range(ring)])


def gather_far(own):
    return shift(own, 3), shift(own, -3)


def gather_near(own, below, above):
    half = own.shape[0] // 2
    from_left = shift(jnp.concatenate([own, above, below[:half]], axis=0), 1)
    from_right = shift(jnp.concatenate([own, below, above[half:]], axis=0), -1)
    return from_left, from_right


def ffn_body(
    me_ref,
    own_ref,
    below_ref,
    above_ref,
    left_ref,
    right_ref,
    gain_ref,
    w_in_ref,
    w_out_ref,
    to_right_ref,
    to_left_ref,
    keep_ref,
    rows_ref,
    sums_ref,
    *,
    block,
):
    me = me_ref[0]
    count, width = own_ref.shape
    half = count // 2
    place = [lax.rem(me + step, RING) for step in range(RING)]
    for start in range(0, count, block):
        at = pl.ds(start, block)
        rows_ref[place[0], at] = own_ref[at]
        rows_ref[place[1], at] = right_ref[at]
        rows_ref[place[7], at] = left_ref[at]
        rows_ref[place[3], at] = above_ref[at]
        rows_ref[place[5], at] = below_ref[at]
        rows_ref[place[2], at] = left_ref[pl.ds(count + start, block)]
        rows_ref[place[6], at] = right_ref[pl.ds(count + start, block)]
        if start < half:
            rows_ref[place[4], at] = left_ref[pl.ds(2 * count + start, block)]
        else:
            rows_ref[place[4], at] = right_ref[pl.ds(2 * count + start - half, block)]
        values = jnp.concatenate([rows_ref[k, at] for k in range(RING)], axis=1)
        values = values.astype(jnp.float32)
        inverse = lax.rsqrt(jnp.mean(values * values, axis=1, keepdims=True) + 1e-05)
        normed = (values * inverse * gain_ref[...]).astype(jnp.bfloat16)
        preact = jnp.dot(normed, w_in_ref[...], preferred_element_type=jnp.float32)
        hidden = jax.nn.gelu(preact, approximate=True).astype(jnp.bfloat16)
        sums = jnp.dot(hidden, w_out_ref[...], preferred_element_type=jnp.float32)
        sums = sums.astype(jnp.bfloat16)
        for k in range(RING):
            sums_ref[k, at] = sums[:, k * width : (k + 1) * width]
        to_right_ref[at] = sums_ref[place[1], at]
        to_right_ref[pl.ds(count + start, block)] = sums_ref[place[6], at]
        to_left_ref[at] = sums_ref[place[7], at]
        to_left_ref[pl.ds(count + start, block)] = sums_ref[place[2], at]
        if start < half:
            to_right_ref[pl.ds(2 * count + start, block)] = sums_ref[place[4], at]
        else:
            to_left_ref[pl.ds(2 * count + start - half, block)] = sums_ref[place[4], at]
        keep_ref[0, at] = sums_ref[place[0], at]
        keep_ref[1, at] = sums_ref[place[3], at]
        keep_ref[2, at] = sums_ref[place[5], at]


def ffn(me, own, below, above, left, right, gain, w_in, w_out):
    count, width = own.shape
    model = RING * width
    vmem = pl.BlockSpec(memory_space=pltpu.VMEM)
    edge = jax.ShapeDtypeStruct((5 * count // 2, width), jnp.bfloat16)
    return pl.pallas_call(
        functools.partial(ffn_body, block=count // 4),
        in_specs=[pl.BlockSpec(memory_space=pltpu.SMEM)] + [vmem] * 8,
        out_specs=[vmem] * 3,
        out_shape=[edge, edge, jax.ShapeDtypeStruct((3, count, width), jnp.bfloat16)],
        scratch_shapes=[
            pltpu.VMEM((RING, count, width), jnp.bfloat16),
            pltpu.VMEM((RING, count, width), jnp.bfloat16),
        ],
        compiler_params=pltpu.CompilerParams(vmem_limit_bytes=32 * 1024 * 1024),
        cost_estimate=pl.CostEstimate(
            flops=4 * count * model * w_in.shape[1],
            transcendentals=count * w_in.shape[1],
            bytes_accessed=4 * count * model + 4 * model * w_in.shape[1],
        ),
    )(me, own, below, above, left, right, gain.reshape(1, model), w_in, w_out)


def scatter_near(to_right, to_left):
    return shift(to_right, 1), shift(to_left, -1)


def scatter_far(keep, from_left, from_right):
    count = keep.shape[1]
    half = count // 2
    keep = keep.astype(jnp.float32)
    from_left = from_left.astype(jnp.float32)
    from_right = from_right.astype(jnp.float32)
    own = keep[0] + from_left[:count] + from_right[:count]
    above = keep[1] + from_right[count : 2 * count]
    above = jnp.concatenate([above[:half] + from_left[2 * count :], above[half:]], axis=0)
    below = keep[2] + from_left[count : 2 * count]
    below = jnp.concatenate([below[:half], below[half:] + from_right[2 * count :]], axis=0)
    first = shift(above.astype(jnp.bfloat16), 3)
    second = shift(below.astype(jnp.bfloat16), -3)
    return own, first, second


def per_device(
    tokens, gain, w_res_in, w_res_out, w_exp_in, w_exp_out, expert_of, slot_of, gate_prob
):
    row_count, feat_width = tokens.shape
    experts = lax.axis_size("expert")
    capacity = max(2, 5 * row_count // (4 * experts))
    slots = experts * capacity
    me = lax.axis_index("mp").astype(jnp.int32).reshape(1)
    slot_id = jnp.where(slot_of >= 0, expert_of * capacity + slot_of, -1)
    slot_index = jnp.arange(slots, dtype=jnp.int32)
    send_table = (slot_index[:, None] == slot_id[None, :]).astype(jnp.bfloat16)
    take_table = (slot_id[:, None] == slot_index[None, :]).astype(jnp.bfloat16)

    def exchange(rows):
        return lax.all_to_all(
            rows.reshape(experts, capacity, feat_width),
            "expert",
            split_axis=0,
            concat_axis=0,
            tiled=True,
        ).reshape(slots, feat_width)

    res_below, res_above = gather_far(tokens)
    outgoing = jnp.dot(send_table, tokens, preferred_element_type=jnp.float32)
    outgoing = outgoing.astype(jnp.bfloat16)
    incoming = exchange(outgoing)
    res_left, res_right = gather_near(tokens, res_below, res_above)
    exp_below, exp_above = gather_far(incoming)
    exp_left, exp_right = gather_near(incoming, exp_below, exp_above)
    res_to_right, res_to_left, res_keep = ffn(
        me, tokens, res_below, res_above, res_left, res_right, gain, w_res_in, w_res_out
    )
    exp_to_right, exp_to_left, exp_keep = ffn(
        me, incoming, exp_below, exp_above, exp_left, exp_right, gain, w_exp_in[0], w_exp_out[0]
    )
    exp_edges = scatter_near(exp_to_right, exp_to_left)
    exp_own, exp_first, exp_second = scatter_far(exp_keep, *exp_edges)
    summed = exp_own + exp_first.astype(jnp.float32) + exp_second.astype(jnp.float32)
    returned = exchange(summed.astype(jnp.bfloat16))
    res_edges = scatter_near(res_to_right, res_to_left)
    res_own, res_first, res_second = scatter_far(res_keep, *res_edges)
    res_sum = res_own + res_first.astype(jnp.float32) + res_second.astype(jnp.float32)
    moe_value = jnp.dot(take_table, returned, preferred_element_type=jnp.float32)
    return (res_sum + gate_prob[:, None] * moe_value).astype(jnp.bfloat16)


def solution(mesh):
    return jax.shard_map(
        per_device,
        mesh=mesh,
        in_specs=(
            P(("groups", "expert"), "mp"),
            P(),
            P(None, "mp"),
            P("mp", None),
            P("expert", None, "mp"),
            P("expert", "mp", None),
            P(("groups", "expert")),
            P(("groups", "expert")),
            P(("groups", "expert")),
        ),
        out_specs=P(("groups", "expert"), "mp"),
        check_vma=False,
    )
```

```python
import functools

import jax
import jax.numpy as jnp
from jax import lax
from jax.experimental import pallas as pl
from jax.experimental.pallas import tpu as pltpu
from jax.sharding import PartitionSpec as P


CHUNKS = 2
RING = 8


def shift(value, step, axis="mp"):
    ring = lax.axis_size(axis)
    return lax.ppermute(value, axis, [(i, (i + step) % ring) for i in range(ring)])


def gather_far(own):
    return shift(own, 3), shift(own, -3)


def gather_near(own, below, above):
    half = own.shape[0] // 2
    from_left = shift(jnp.concatenate([own, above, below[:half]], axis=0), 1)
    from_right = shift(jnp.concatenate([own, below, above[half:]], axis=0), -1)
    return from_left, from_right


def ffn_body(
    me_ref,
    own_ref,
    below_ref,
    above_ref,
    left_ref,
    right_ref,
    gain_ref,
    w_in_ref,
    w_out_ref,
    to_right_ref,
    to_left_ref,
    keep_ref,
    rows_ref,
    sums_ref,
    *,
    block,
):
    me = me_ref[0]
    count, width = own_ref.shape
    half = count // 2
    place = [lax.rem(me + step, RING) for step in range(RING)]
    for start in range(0, count, block):
        at = pl.ds(start, block)
        rows_ref[place[0], at] = own_ref[at]
        rows_ref[place[1], at] = right_ref[at]
        rows_ref[place[7], at] = left_ref[at]
        rows_ref[place[3], at] = above_ref[at]
        rows_ref[place[5], at] = below_ref[at]
        rows_ref[place[2], at] = left_ref[pl.ds(count + start, block)]
        rows_ref[place[6], at] = right_ref[pl.ds(count + start, block)]
        if start < half:
            rows_ref[place[4], at] = left_ref[pl.ds(2 * count + start, block)]
        else:
            rows_ref[place[4], at] = right_ref[pl.ds(2 * count + start - half, block)]
        values = jnp.concatenate([rows_ref[k, at] for k in range(RING)], axis=1)
        values = values.astype(jnp.float32)
        inverse = lax.rsqrt(jnp.mean(values * values, axis=1, keepdims=True) + 1e-05)
        normed = (values * inverse * gain_ref[...]).astype(jnp.bfloat16)
        preact = jnp.dot(normed, w_in_ref[...], preferred_element_type=jnp.float32)
        hidden = jax.nn.gelu(preact, approximate=True).astype(jnp.bfloat16)
        sums = jnp.dot(hidden, w_out_ref[...], preferred_element_type=jnp.float32)
        sums = sums.astype(jnp.bfloat16)
        for k in range(RING):
            sums_ref[k, at] = sums[:, k * width : (k + 1) * width]
        to_right_ref[at] = sums_ref[place[1], at]
        to_right_ref[pl.ds(count + start, block)] = sums_ref[place[6], at]
        to_left_ref[at] = sums_ref[place[7], at]
        to_left_ref[pl.ds(count + start, block)] = sums_ref[place[2], at]
        if start < half:
            to_right_ref[pl.ds(2 * count + start, block)] = sums_ref[place[4], at]
        else:
            to_left_ref[pl.ds(2 * count + start - half, block)] = sums_ref[place[4], at]
        keep_ref[0, at] = sums_ref[place[0], at]
        keep_ref[1, at] = sums_ref[place[3], at]
        keep_ref[2, at] = sums_ref[place[5], at]


def ffn(me, own, below, above, left, right, gain, w_in, w_out):
    count, width = own.shape
    model = RING * width
    vmem = pl.BlockSpec(memory_space=pltpu.VMEM)
    edge = jax.ShapeDtypeStruct((5 * count // 2, width), jnp.bfloat16)
    return pl.pallas_call(
        functools.partial(ffn_body, block=count // 4),
        in_specs=[pl.BlockSpec(memory_space=pltpu.SMEM)] + [vmem] * 8,
        out_specs=[vmem] * 3,
        out_shape=[edge, edge, jax.ShapeDtypeStruct((3, count, width), jnp.bfloat16)],
        scratch_shapes=[
            pltpu.VMEM((RING, count, width), jnp.bfloat16),
            pltpu.VMEM((RING, count, width), jnp.bfloat16),
        ],
        compiler_params=pltpu.CompilerParams(vmem_limit_bytes=32 * 1024 * 1024),
        cost_estimate=pl.CostEstimate(
            flops=4 * count * model * w_in.shape[1],
            transcendentals=count * w_in.shape[1],
            bytes_accessed=4 * count * model + 4 * model * w_in.shape[1],
        ),
    )(me, own, below, above, left, right, gain.reshape(1, model), w_in, w_out)


def scatter_near(to_right, to_left):
    return shift(to_right, 1), shift(to_left, -1)


def scatter_far(keep, from_left, from_right):
    count = keep.shape[1]
    half = count // 2
    keep = keep.astype(jnp.float32)
    from_left = from_left.astype(jnp.float32)
    from_right = from_right.astype(jnp.float32)
    own = keep[0] + from_left[:count] + from_right[:count]
    above = keep[1] + from_right[count : 2 * count]
    above = jnp.concatenate([above[:half] + from_left[2 * count :], above[half:]], axis=0)
    below = keep[2] + from_left[count : 2 * count]
    below = jnp.concatenate([below[:half], below[half:] + from_right[2 * count :]], axis=0)
    first = shift(above.astype(jnp.bfloat16), 3)
    second = shift(below.astype(jnp.bfloat16), -3)
    return own, first, second


def per_device(
    tokens, gain, w_res_in, w_res_out, w_exp_in, w_exp_out, expert_of, slot_of, gate_prob
):
    row_count, feat_width = tokens.shape
    experts = lax.axis_size("expert")
    capacity = max(2, 5 * row_count // (4 * experts))
    slots = experts * capacity
    me = lax.axis_index("mp").astype(jnp.int32).reshape(1)
    slot_id = jnp.where(slot_of >= 0, expert_of * capacity + slot_of, -1)
    slot_index = jnp.arange(slots, dtype=jnp.int32)
    send_table = (slot_index[:, None] == slot_id[None, :]).astype(jnp.bfloat16)
    take_table = (slot_id[:, None] == slot_index[None, :]).astype(jnp.bfloat16)

    def exchange(rows):
        return lax.all_to_all(
            rows.reshape(experts, capacity, feat_width),
            "expert",
            split_axis=0,
            concat_axis=0,
            tiled=True,
        ).reshape(slots, feat_width)

    res_below = shift(tokens, 3)
    outgoing = jnp.dot(send_table, tokens, preferred_element_type=jnp.float32)
    outgoing = outgoing.astype(jnp.bfloat16)
    incoming = exchange(outgoing)
    res_above = shift(tokens, -3)
    res_left, res_right = gather_near(tokens, res_below, res_above)
    res_to_right, res_to_left, res_keep = ffn(
        me, tokens, res_below, res_above, res_left, res_right, gain, w_res_in, w_res_out
    )

    chunk = slots // CHUNKS
    summed = []
    for c in range(CHUNKS):
        rows = incoming[c * chunk : (c + 1) * chunk]
        below, above = gather_far(rows)
        left, right = gather_near(rows, below, above)
        to_right, to_left, keep = ffn(
            me, rows, below, above, left, right, gain, w_exp_in[0], w_exp_out[0]
        )
        edges = scatter_near(to_right, to_left)
        own, first, second = scatter_far(keep, *edges)
        own = own + first.astype(jnp.float32) + second.astype(jnp.float32)
        summed.append(own.astype(jnp.bfloat16))

    returned = exchange(jnp.concatenate(summed, axis=0))
    res_edges = scatter_near(res_to_right, res_to_left)
    res_own, res_first, res_second = scatter_far(res_keep, *res_edges)
    res_sum = res_own + res_first.astype(jnp.float32) + res_second.astype(jnp.float32)
    moe_value = jnp.dot(take_table, returned, preferred_element_type=jnp.float32)
    return (res_sum + gate_prob[:, None] * moe_value).astype(jnp.bfloat16)


def solution(mesh):
    return jax.shard_map(
        per_device,
        mesh=mesh,
        in_specs=(
            P(("groups", "expert"), "mp"),
            P(),
            P(None, "mp"),
            P("mp", None),
            P("expert", None, "mp"),
            P("expert", "mp", None),
            P(("groups", "expert")),
            P(("groups", "expert")),
            P(("groups", "expert")),
        ),
        out_specs=P(("groups", "expert"), "mp"),
        check_vma=False,
    )
```

```python
import functools

import jax
import jax.numpy as jnp
from jax import lax
from jax.experimental import pallas as pl
from jax.experimental.pallas import tpu as pltpu
from jax.sharding import PartitionSpec as P


CHUNKS = 2
RING = 8


def shift(value, step, axis="mp"):
    ring = lax.axis_size(axis)
    return lax.ppermute(value, axis, [(i, (i + step) % ring) for i in range(ring)])


def gather_far(own):
    return shift(own, 3), shift(own, -3)


def gather_near(own, below, above):
    half = own.shape[0] // 2
    from_left = shift(jnp.concatenate([own, above, below[:half]], axis=0), 1)
    from_right = shift(jnp.concatenate([own, below, above[half:]], axis=0), -1)
    return from_left, from_right


def mlp(values, gain_ref, w_in_ref, w_out_ref):
    values = values.astype(jnp.float32)
    inverse = lax.rsqrt(jnp.mean(values * values, axis=1, keepdims=True) + 1e-05)
    normed = (values * inverse * gain_ref[...]).astype(jnp.bfloat16)
    preact = jnp.dot(normed, w_in_ref[...], preferred_element_type=jnp.float32)
    hidden = jax.nn.gelu(preact, approximate=True).astype(jnp.bfloat16)
    sums = jnp.dot(hidden, w_out_ref[...], preferred_element_type=jnp.float32)
    return sums.astype(jnp.bfloat16)


def estimate(count, model, hidden):
    return pl.CostEstimate(
        flops=4 * count * model * hidden,
        transcendentals=count * hidden,
        bytes_accessed=4 * count * model + 4 * model * hidden,
    )


def ffn_body(
    me_ref,
    own_ref,
    below_ref,
    above_ref,
    left_ref,
    right_ref,
    gain_ref,
    w_in_ref,
    w_out_ref,
    to_right_ref,
    to_left_ref,
    keep_ref,
    rows_ref,
    sums_ref,
    *,
    block,
):
    me = me_ref[0]
    count, width = own_ref.shape
    half = count // 2
    place = [lax.rem(me + step, RING) for step in range(RING)]
    for start in range(0, count, block):
        at = pl.ds(start, block)
        rows_ref[place[0], at] = own_ref[at]
        rows_ref[place[1], at] = right_ref[at]
        rows_ref[place[7], at] = left_ref[at]
        rows_ref[place[3], at] = above_ref[at]
        rows_ref[place[5], at] = below_ref[at]
        rows_ref[place[2], at] = left_ref[pl.ds(count + start, block)]
        rows_ref[place[6], at] = right_ref[pl.ds(count + start, block)]
        if start < half:
            rows_ref[place[4], at] = left_ref[pl.ds(2 * count + start, block)]
        else:
            rows_ref[place[4], at] = right_ref[pl.ds(2 * count + start - half, block)]
        values = jnp.concatenate([rows_ref[k, at] for k in range(RING)], axis=1)
        sums = mlp(values, gain_ref, w_in_ref, w_out_ref)
        for k in range(RING):
            sums_ref[k, at] = sums[:, k * width : (k + 1) * width]
        to_right_ref[at] = sums_ref[place[1], at]
        to_right_ref[pl.ds(count + start, block)] = sums_ref[place[6], at]
        to_left_ref[at] = sums_ref[place[7], at]
        to_left_ref[pl.ds(count + start, block)] = sums_ref[place[2], at]
        if start < half:
            to_right_ref[pl.ds(2 * count + start, block)] = sums_ref[place[4], at]
        else:
            to_left_ref[pl.ds(2 * count + start - half, block)] = sums_ref[place[4], at]
        keep_ref[0, at] = sums_ref[place[0], at]
        keep_ref[1, at] = sums_ref[place[3], at]
        keep_ref[2, at] = sums_ref[place[5], at]


def ffn(me, own, below, above, left, right, gain, w_in, w_out):
    count, width = own.shape
    model = RING * width
    vmem = pl.BlockSpec(memory_space=pltpu.VMEM)
    edge = jax.ShapeDtypeStruct((5 * count // 2, width), jnp.bfloat16)
    return pl.pallas_call(
        functools.partial(ffn_body, block=count // 4),
        in_specs=[pl.BlockSpec(memory_space=pltpu.SMEM)] + [vmem] * 8,
        out_specs=[vmem] * 3,
        out_shape=[edge, edge, jax.ShapeDtypeStruct((3, count, width), jnp.bfloat16)],
        scratch_shapes=[
            pltpu.VMEM((RING, count, width), jnp.bfloat16),
            pltpu.VMEM((RING, count, width), jnp.bfloat16),
        ],
        compiler_params=pltpu.CompilerParams(vmem_limit_bytes=32 * 1024 * 1024),
        cost_estimate=estimate(count, model, w_in.shape[1]),
    )(me, own, below, above, left, right, gain.reshape(1, model), w_in, w_out)


def res_body(rows_ref, gain_ref, w_in_ref, w_out_ref, out_ref, *, block):
    parts, count, width = rows_ref.shape
    for start in range(0, count, block):
        at = pl.ds(start, block)
        values = jnp.concatenate([rows_ref[k, at] for k in range(parts)], axis=1)
        sums = mlp(values, gain_ref, w_in_ref, w_out_ref)
        for k in range(parts):
            out_ref[k, at] = sums[:, k * width : (k + 1) * width]


def res_ffn(rows, gain, w_in, w_out):
    parts, count, width = rows.shape
    model = parts * width
    vmem = pl.BlockSpec(memory_space=pltpu.VMEM)
    return pl.pallas_call(
        functools.partial(res_body, block=count // 4),
        in_specs=[vmem] * 4,
        out_specs=vmem,
        out_shape=jax.ShapeDtypeStruct(rows.shape, jnp.bfloat16),
        compiler_params=pltpu.CompilerParams(vmem_limit_bytes=32 * 1024 * 1024),
        cost_estimate=estimate(count, model, w_in.shape[1]),
        name="res",
    )(rows, gain.reshape(1, model), w_in, w_out)


def scatter_near(to_right, to_left):
    return shift(to_right, 1), shift(to_left, -1)


def scatter_far(keep, from_left, from_right):
    count = keep.shape[1]
    half = count // 2
    keep = keep.astype(jnp.float32)
    from_left = from_left.astype(jnp.float32)
    from_right = from_right.astype(jnp.float32)
    own = keep[0] + from_left[:count] + from_right[:count]
    above = keep[1] + from_right[count : 2 * count]
    above = jnp.concatenate([above[:half] + from_left[2 * count :], above[half:]], axis=0)
    below = keep[2] + from_left[count : 2 * count]
    below = jnp.concatenate([below[:half], below[half:] + from_right[2 * count :]], axis=0)
    first = shift(above.astype(jnp.bfloat16), 3)
    second = shift(below.astype(jnp.bfloat16), -3)
    return own, first, second


def per_device(
    tokens, gain, w_res_in, w_res_out, w_exp_in, w_exp_out, expert_of, slot_of, gate_prob
):
    row_count, feat_width = tokens.shape
    experts = lax.axis_size("expert")
    capacity = max(2, 5 * row_count // (4 * experts))
    slots = experts * capacity
    me = lax.axis_index("mp").astype(jnp.int32).reshape(1)
    slot_id = jnp.where(slot_of >= 0, expert_of * capacity + slot_of, -1)
    slot_index = jnp.arange(slots, dtype=jnp.int32)
    send_table = (slot_index[:, None] == slot_id[None, :]).astype(jnp.bfloat16)
    take_table = (slot_id[:, None] == slot_index[None, :]).astype(jnp.bfloat16)

    def exchange(rows):
        return lax.all_to_all(
            rows.reshape(experts, capacity, feat_width),
            "expert",
            split_axis=0,
            concat_axis=0,
            tiled=True,
        ).reshape(slots, feat_width)

    res_rows = lax.all_gather(tokens, "mp", axis=0)
    outgoing = jnp.dot(send_table, tokens, preferred_element_type=jnp.float32)
    outgoing = outgoing.astype(jnp.bfloat16)
    incoming = exchange(outgoing)
    res_parts = res_ffn(res_rows, gain, w_res_in, w_res_out)
    res_sum = lax.psum_scatter(res_parts, "mp", scatter_dimension=0, tiled=False)
    res_sum = res_sum.astype(jnp.float32)

    chunk = slots // CHUNKS
    summed = []
    for c in range(CHUNKS):
        rows = incoming[c * chunk : (c + 1) * chunk]
        below, above = gather_far(rows)
        left, right = gather_near(rows, below, above)
        to_right, to_left, keep = ffn(
            me, rows, below, above, left, right, gain, w_exp_in[0], w_exp_out[0]
        )
        edges = scatter_near(to_right, to_left)
        own, first, second = scatter_far(keep, *edges)
        own = own + first.astype(jnp.float32) + second.astype(jnp.float32)
        summed.append(own.astype(jnp.bfloat16))

    returned = exchange(jnp.concatenate(summed, axis=0))
    moe_value = jnp.dot(take_table, returned, preferred_element_type=jnp.float32)
    return (res_sum + gate_prob[:, None] * moe_value).astype(jnp.bfloat16)


def solution(mesh):
    return jax.shard_map(
        per_device,
        mesh=mesh,
        in_specs=(
            P(("groups", "expert"), "mp"),
            P(),
            P(None, "mp"),
            P("mp", None),
            P("expert", None, "mp"),
            P("expert", "mp", None),
            P(("groups", "expert")),
            P(("groups", "expert")),
            P(("groups", "expert")),
        ),
        out_specs=P(("groups", "expert"), "mp"),
        check_vma=False,
    )
```

```python
import functools

import jax
import jax.numpy as jnp
from jax import lax
from jax.experimental import pallas as pl
from jax.experimental.pallas import tpu as pltpu
from jax.sharding import PartitionSpec as P


RING = 8


def shift(value, step):
    experts, ring = lax.axis_size("expert"), lax.axis_size("mp")
    pairs = []
    for e in range(experts):
        along = step if e % 2 == 0 else -step
        pairs += [(e * ring + i, e * ring + (i + along) % ring) for i in range(ring)]
    return lax.ppermute(value, ("expert", "mp"), pairs)


def gather_far(own):
    return shift(own, 3), shift(own, -3)


def gather_near(own, below, above):
    half = own.shape[0] // 2
    from_left = shift(jnp.concatenate([own, above, below[:half]], axis=0), 1)
    from_right = shift(jnp.concatenate([own, below, above[half:]], axis=0), -1)
    return from_left, from_right


def ffn_body(
    me_ref,
    own_ref,
    below_ref,
    above_ref,
    left_ref,
    right_ref,
    gain_ref,
    w_in_ref,
    w_out_ref,
    to_right_ref,
    to_left_ref,
    keep_ref,
    rows_ref,
    sums_ref,
    *,
    block,
):
    me, sign = me_ref[0], me_ref[1]
    count, width = own_ref.shape
    half = count // 2
    place = [lax.rem(me + RING + sign * step, RING) for step in range(RING)]
    for start in range(0, count, block):
        at = pl.ds(start, block)
        rows_ref[place[0], at] = own_ref[at]
        rows_ref[place[1], at] = right_ref[at]
        rows_ref[place[7], at] = left_ref[at]
        rows_ref[place[3], at] = above_ref[at]
        rows_ref[place[5], at] = below_ref[at]
        rows_ref[place[2], at] = left_ref[pl.ds(count + start, block)]
        rows_ref[place[6], at] = right_ref[pl.ds(count + start, block)]
        if start < half:
            rows_ref[place[4], at] = left_ref[pl.ds(2 * count + start, block)]
        else:
            rows_ref[place[4], at] = right_ref[pl.ds(2 * count + start - half, block)]
        values = jnp.concatenate([rows_ref[k, at] for k in range(RING)], axis=1)
        values = values.astype(jnp.float32)
        inverse = lax.rsqrt(jnp.mean(values * values, axis=1, keepdims=True) + 1e-05)
        normed = (values * inverse * gain_ref[...]).astype(jnp.bfloat16)
        preact = jnp.dot(normed, w_in_ref[...], preferred_element_type=jnp.float32)
        hidden = jax.nn.gelu(preact, approximate=True).astype(jnp.bfloat16)
        sums = jnp.dot(hidden, w_out_ref[...], preferred_element_type=jnp.float32)
        sums = sums.astype(jnp.bfloat16)
        for k in range(RING):
            sums_ref[k, at] = sums[:, k * width : (k + 1) * width]
        to_right_ref[at] = sums_ref[place[1], at]
        to_right_ref[pl.ds(count + start, block)] = sums_ref[place[6], at]
        to_left_ref[at] = sums_ref[place[7], at]
        to_left_ref[pl.ds(count + start, block)] = sums_ref[place[2], at]
        if start < half:
            to_right_ref[pl.ds(2 * count + start, block)] = sums_ref[place[4], at]
        else:
            to_left_ref[pl.ds(2 * count + start - half, block)] = sums_ref[place[4], at]
        keep_ref[0, at] = sums_ref[place[0], at]
        keep_ref[1, at] = sums_ref[place[3], at]
        keep_ref[2, at] = sums_ref[place[5], at]


def ffn(me, own, below, above, left, right, gain, w_in, w_out):
    count, width = own.shape
    model = RING * width
    vmem = pl.BlockSpec(memory_space=pltpu.VMEM)
    edge = jax.ShapeDtypeStruct((5 * count // 2, width), jnp.bfloat16)
    return pl.pallas_call(
        functools.partial(ffn_body, block=count // 4),
        in_specs=[pl.BlockSpec(memory_space=pltpu.SMEM)] + [vmem] * 8,
        out_specs=[vmem] * 3,
        out_shape=[edge, edge, jax.ShapeDtypeStruct((3, count, width), jnp.bfloat16)],
        scratch_shapes=[
            pltpu.VMEM((RING, count, width), jnp.bfloat16),
            pltpu.VMEM((RING, count, width), jnp.bfloat16),
        ],
        compiler_params=pltpu.CompilerParams(vmem_limit_bytes=32 * 1024 * 1024),
        cost_estimate=pl.CostEstimate(
            flops=4 * count * model * w_in.shape[1],
            transcendentals=count * w_in.shape[1],
            bytes_accessed=4 * count * model + 4 * model * w_in.shape[1],
        ),
    )(me, own, below, above, left, right, gain.reshape(1, model), w_in, w_out)


def scatter_near(to_right, to_left):
    return shift(to_right, 1), shift(to_left, -1)


def scatter_far(keep, from_left, from_right):
    count = keep.shape[1]
    half = count // 2
    keep = keep.astype(jnp.float32)
    from_left = from_left.astype(jnp.float32)
    from_right = from_right.astype(jnp.float32)
    own = keep[0] + from_left[:count] + from_right[:count]
    above = keep[1] + from_right[count : 2 * count]
    above = jnp.concatenate([above[:half] + from_left[2 * count :], above[half:]], axis=0)
    below = keep[2] + from_left[count : 2 * count]
    below = jnp.concatenate([below[:half], below[half:] + from_right[2 * count :]], axis=0)
    first = shift(above.astype(jnp.bfloat16), 3)
    second = shift(below.astype(jnp.bfloat16), -3)
    return own, first, second


def per_device(
    tokens, gain, w_res_in, w_res_out, w_exp_in, w_exp_out, expert_of, slot_of, gate_prob
):
    row_count, feat_width = tokens.shape
    experts = lax.axis_size("expert")
    capacity = max(2, 5 * row_count // (4 * experts))
    slots = experts * capacity
    odd = lax.rem(lax.axis_index("expert"), 2)
    me = jnp.stack([lax.axis_index("mp"), 1 - 2 * odd]).astype(jnp.int32)
    slot_id = jnp.where(slot_of >= 0, expert_of * capacity + slot_of, -1)
    slot_index = jnp.arange(slots, dtype=jnp.int32)
    send_table = (slot_index[:, None] == slot_id[None, :]).astype(jnp.bfloat16)
    take_table = (slot_id[:, None] == slot_index[None, :]).astype(jnp.bfloat16)

    def exchange(rows):
        return lax.all_to_all(
            rows.reshape(experts, capacity, feat_width),
            "expert",
            split_axis=0,
            concat_axis=0,
            tiled=True,
        ).reshape(slots, feat_width)

    res_below, res_above = gather_far(tokens)
    outgoing = jnp.dot(send_table, tokens, preferred_element_type=jnp.float32)
    outgoing = outgoing.astype(jnp.bfloat16)
    incoming = exchange(outgoing)
    res_left, res_right = gather_near(tokens, res_below, res_above)
    exp_below, exp_above = gather_far(incoming)
    exp_left, exp_right = gather_near(incoming, exp_below, exp_above)
    res_to_right, res_to_left, res_keep = ffn(
        me, tokens, res_below, res_above, res_left, res_right, gain, w_res_in, w_res_out
    )
    exp_to_right, exp_to_left, exp_keep = ffn(
        me, incoming, exp_below, exp_above, exp_left, exp_right, gain, w_exp_in[0], w_exp_out[0]
    )
    exp_edges = scatter_near(exp_to_right, exp_to_left)
    exp_own, exp_first, exp_second = scatter_far(exp_keep, *exp_edges)
    summed = exp_own + exp_first.astype(jnp.float32) + exp_second.astype(jnp.float32)
    returned = exchange(summed.astype(jnp.bfloat16))
    res_edges = scatter_near(res_to_right, res_to_left)
    res_own, res_first, res_second = scatter_far(res_keep, *res_edges)
    res_sum = res_own + res_first.astype(jnp.float32) + res_second.astype(jnp.float32)
    moe_value = jnp.dot(take_table, returned, preferred_element_type=jnp.float32)
    return (res_sum + gate_prob[:, None] * moe_value).astype(jnp.bfloat16)


def solution(mesh):
    return jax.shard_map(
        per_device,
        mesh=mesh,
        in_specs=(
            P(("groups", "expert"), "mp"),
            P(),
            P(None, "mp"),
            P("mp", None),
            P("expert", None, "mp"),
            P("expert", "mp", None),
            P(("groups", "expert")),
            P(("groups", "expert")),
            P(("groups", "expert")),
        ),
        out_specs=P(("groups", "expert"), "mp"),
        check_vma=False,
    )
```

```python
import functools

import jax
import jax.numpy as jnp
from jax import lax
from jax.experimental import pallas as pl
from jax.experimental.pallas import tpu as pltpu
from jax.sharding import PartitionSpec as P


RING = 8


def shift(value, step, axis="mp"):
    ring = lax.axis_size(axis)
    return lax.ppermute(value, axis, [(i, (i + step) % ring) for i in range(ring)])


def gather_far(own):
    return shift(own, 3), shift(own, -3)


def gather_near(own, below, above):
    half = own.shape[0] // 2
    from_left = shift(jnp.concatenate([own, above, below[:half]], axis=0), 1)
    from_right = shift(jnp.concatenate([own, below, above[half:]], axis=0), -1)
    return from_left, from_right


def branch(
    me,
    own_ref,
    below_ref,
    above_ref,
    left_ref,
    right_ref,
    gain_ref,
    w_in_ref,
    w_out_ref,
    to_right_ref,
    to_left_ref,
    keep_ref,
    rows_ref,
    sums_ref,
    block,
    base,
):
    count, width = own_ref.shape
    half = count // 2
    place = [lax.rem(me + step, RING) for step in range(RING)]
    for start in range(0, count, block):
        at = pl.ds(start, block)
        first = pl.ds(base + start, block)
        second = pl.ds(base + count + start, block)
        rows_ref[place[0], at] = own_ref[at]
        rows_ref[place[1], at] = right_ref[at]
        rows_ref[place[7], at] = left_ref[at]
        rows_ref[place[3], at] = above_ref[at]
        rows_ref[place[5], at] = below_ref[at]
        rows_ref[place[2], at] = left_ref[pl.ds(count + start, block)]
        rows_ref[place[6], at] = right_ref[pl.ds(count + start, block)]
        if start < half:
            rows_ref[place[4], at] = left_ref[pl.ds(2 * count + start, block)]
        else:
            rows_ref[place[4], at] = right_ref[pl.ds(2 * count + start - half, block)]
        values = jnp.concatenate([rows_ref[k, at] for k in range(RING)], axis=1)
        values = values.astype(jnp.float32)
        inverse = lax.rsqrt(jnp.mean(values * values, axis=1, keepdims=True) + 1e-05)
        normed = (values * inverse * gain_ref[...]).astype(jnp.bfloat16)
        preact = jnp.dot(normed, w_in_ref[...], preferred_element_type=jnp.float32)
        hidden = jax.nn.gelu(preact, approximate=True).astype(jnp.bfloat16)
        sums = jnp.dot(hidden, w_out_ref[...], preferred_element_type=jnp.float32)
        sums = sums.astype(jnp.bfloat16)
        for k in range(RING):
            sums_ref[k, at] = sums[:, k * width : (k + 1) * width]
        to_right_ref[first] = sums_ref[place[1], at]
        to_right_ref[second] = sums_ref[place[6], at]
        to_left_ref[first] = sums_ref[place[7], at]
        to_left_ref[second] = sums_ref[place[2], at]
        if start < half:
            to_right_ref[pl.ds(base + 2 * count + start, block)] = sums_ref[place[4], at]
        else:
            third = pl.ds(base + 2 * count + start - half, block)
            to_left_ref[third] = sums_ref[place[4], at]
        keep_ref[0, at] = sums_ref[place[0], at]
        keep_ref[1, at] = sums_ref[place[3], at]
        keep_ref[2, at] = sums_ref[place[5], at]


def ffn_body(me_ref, *refs, block):
    branch(me_ref[0], *refs, block, 0)


def pair_body(me_ref, *refs, block, later_block):
    own, below, above, left, right, gain, w_in, w_out = refs[:8]
    sources = refs[8:15]
    to_right, to_left, keep, later_keep = refs[15:19]
    rows, sums, later_rows, later_sums = refs[19:23]
    targets = refs[23:30]
    done = refs[30]
    copies = [
        pltpu.make_async_copy(source, target, done.at[n])
        for n, (source, target) in enumerate(zip(sources, targets))
    ]
    for copy in copies:
        copy.start()
    me = me_ref[0]
    branch(
        me,
        own,
        below,
        above,
        left,
        right,
        gain,
        w_in,
        w_out,
        to_right,
        to_left,
        keep,
        rows,
        sums,
        block,
        0,
    )
    for copy in copies:
        copy.wait()
    branch(
        me,
        *targets[:5],
        gain,
        *targets[5:],
        to_right,
        to_left,
        later_keep,
        later_rows,
        later_sums,
        later_block,
        5 * own.shape[0] // 2,
    )


def sums_of(count, width):
    return jax.ShapeDtypeStruct((3, count, width), jnp.bfloat16)


def tiles_of(count, width):
    return pltpu.VMEM((RING, count, width), jnp.bfloat16)


def estimate(count, model, hidden):
    return pl.CostEstimate(
        flops=4 * count * model * hidden,
        transcendentals=count * hidden,
        bytes_accessed=4 * count * model + 4 * model * hidden,
    )


def ffn(me, pieces, gain, w_in, w_out):
    count, width = pieces[0].shape
    model = RING * width
    vmem = pl.BlockSpec(memory_space=pltpu.VMEM)
    edge = jax.ShapeDtypeStruct((5 * count // 2, width), jnp.bfloat16)
    return pl.pallas_call(
        functools.partial(ffn_body, block=count // 4),
        in_specs=[pl.BlockSpec(memory_space=pltpu.SMEM)] + [vmem] * 8,
        out_specs=[vmem] * 3,
        out_shape=[edge, edge, sums_of(count, width)],
        scratch_shapes=[tiles_of(count, width)] * 2,
        compiler_params=pltpu.CompilerParams(vmem_limit_bytes=32 * 1024 * 1024),
        cost_estimate=estimate(count, model, w_in.shape[1]),
        name="exp",
    )(me, *pieces, gain.reshape(1, model), w_in, w_out)


def ffn_pair(me, pieces, gain, w_in, w_out, later_pieces, later_in, later_out):
    count, width = pieces[0].shape
    later = later_pieces[0].shape[0]
    model = RING * width
    vmem = pl.BlockSpec(memory_space=pltpu.VMEM)
    anywhere = pl.BlockSpec(memory_space=pl.ANY)
    edge = jax.ShapeDtypeStruct((5 * (count + later) // 2, width), jnp.bfloat16)
    operands = [*later_pieces, later_in, later_out]
    return pl.pallas_call(
        functools.partial(pair_body, block=count // 4, later_block=later // 4),
        in_specs=[pl.BlockSpec(memory_space=pltpu.SMEM)] + [vmem] * 8 + [anywhere] * 7,
        out_specs=[vmem] * 4,
        out_shape=[edge, edge, sums_of(count, width), sums_of(later, width)],
        scratch_shapes=[tiles_of(count, width)] * 2
        + [tiles_of(later, width)] * 2
        + [pltpu.VMEM(value.shape, value.dtype) for value in operands]
        + [pltpu.SemaphoreType.DMA((7,))],
        compiler_params=pltpu.CompilerParams(vmem_limit_bytes=40 * 1024 * 1024),
        cost_estimate=estimate(count + later, model, w_in.shape[1]),
        name="pair",
    )(me, *pieces, gain.reshape(1, model), w_in, w_out, *operands)


def scatter_near(to_right, to_left):
    return shift(to_right, 1), shift(to_left, -1)


def scatter_far(keep, from_left, from_right, base=0):
    count = keep.shape[1]
    half = count // 2
    one, two = base + count, base + 2 * count

    def wide(value):
        return value.astype(jnp.float32)

    own = wide(keep[0]) + wide(from_left[base:one]) + wide(from_right[base:one])
    above = wide(keep[1]) + wide(from_right[one:two])
    to_above = jnp.concatenate(
        [above[:half] + wide(from_left[two : two + half]), above[half:]], axis=0
    )
    below = wide(keep[2]) + wide(from_left[one:two])
    to_below = jnp.concatenate(
        [below[:half], below[half:] + wide(from_right[two : two + half])], axis=0
    )
    first = shift(to_above.astype(jnp.bfloat16), 3)
    second = shift(to_below.astype(jnp.bfloat16), -3)
    return own, first, second


def per_device(
    tokens, gain, w_res_in, w_res_out, w_exp_in, w_exp_out, expert_of, slot_of, gate_prob
):
    row_count, feat_width = tokens.shape
    experts = lax.axis_size("expert")
    capacity = max(2, 5 * row_count // (4 * experts))
    slots = experts * capacity
    me = lax.axis_index("mp").astype(jnp.int32).reshape(1)
    slot_id = jnp.where(slot_of >= 0, expert_of * capacity + slot_of, -1)
    slot_index = jnp.arange(slots, dtype=jnp.int32)
    send_table = (slot_index[:, None] == slot_id[None, :]).astype(jnp.bfloat16)
    take_table = (slot_id[:, None] == slot_index[None, :]).astype(jnp.bfloat16)

    def exchange(rows):
        return lax.all_to_all(
            rows.reshape(experts, capacity, feat_width),
            "expert",
            split_axis=0,
            concat_axis=0,
            tiled=True,
        ).reshape(slots, feat_width)

    res_below = shift(tokens, 3)
    outgoing = jnp.dot(send_table, tokens, preferred_element_type=jnp.float32)
    outgoing = outgoing.astype(jnp.bfloat16)
    incoming = exchange(outgoing)
    res_above = shift(tokens, -3)
    res_left, res_right = gather_near(tokens, res_below, res_above)
    res_pieces = (tokens, res_below, res_above, res_left, res_right)
    chunk = slots // 2
    pieces = []
    for c in range(2):
        rows = incoming[c * chunk : (c + 1) * chunk]
        below, above = gather_far(rows)
        left, right = gather_near(rows, below, above)
        pieces.append((rows, below, above, left, right))
    to_right, to_left, keep_0 = ffn(me, pieces[0], gain, w_exp_in[0], w_exp_out[0])
    edges_0 = scatter_near(to_right, to_left)
    to_right, to_left, keep_1, res_keep = ffn_pair(
        me,
        pieces[1],
        gain,
        w_exp_in[0],
        w_exp_out[0],
        res_pieces,
        w_res_in,
        w_res_out,
    )
    edges_1 = scatter_near(to_right, to_left)
    summed = []
    for keep, edges in ((keep_0, edges_0), (keep_1, edges_1)):
        own, first, second = scatter_far(keep, *edges)
        own = own + first.astype(jnp.float32) + second.astype(jnp.float32)
        summed.append(own.astype(jnp.bfloat16))

    returned = exchange(jnp.concatenate(summed, axis=0))
    res_own, res_first, res_second = scatter_far(res_keep, *edges_1, 5 * chunk // 2)
    res_sum = res_own + res_first.astype(jnp.float32) + res_second.astype(jnp.float32)
    moe_value = jnp.dot(take_table, returned, preferred_element_type=jnp.float32)
    return (res_sum + gate_prob[:, None] * moe_value).astype(jnp.bfloat16)


def solution(mesh):
    return jax.shard_map(
        per_device,
        mesh=mesh,
        in_specs=(
            P(("groups", "expert"), "mp"),
            P(),
            P(None, "mp"),
            P("mp", None),
            P("expert", None, "mp"),
            P("expert", "mp", None),
            P(("groups", "expert")),
            P(("groups", "expert")),
            P(("groups", "expert")),
        ),
        out_specs=P(("groups", "expert"), "mp"),
        check_vma=False,
    )
```

```python
import functools

import jax
import jax.numpy as jnp
from jax import lax
from jax.experimental import pallas as pl
from jax.experimental.pallas import tpu as pltpu
from jax.sharding import PartitionSpec as P


RING = 8


def shift(value, step, axis="mp"):
    ring = lax.axis_size(axis)
    return lax.ppermute(value, axis, [(i, (i + step) % ring) for i in range(ring)])


def gather_far(own):
    return shift(own, 3), shift(own, -3)


def gather_near(own, below, above):
    half = own.shape[0] // 2
    from_left = shift(jnp.concatenate([own, above, below[:half]], axis=0), 1)
    from_right = shift(jnp.concatenate([own, below, above[half:]], axis=0), -1)
    return from_left, from_right


def branch(
    me,
    own_ref,
    below_ref,
    above_ref,
    left_ref,
    right_ref,
    gain_ref,
    w_in_ref,
    w_out_ref,
    to_right_ref,
    to_left_ref,
    keep_ref,
    rows_ref,
    sums_ref,
    block,
):
    count, width = own_ref.shape
    half = count // 2
    place = [lax.rem(me + step, RING) for step in range(RING)]
    for start in range(0, count, block):
        at = pl.ds(start, block)
        second = pl.ds(count + start, block)
        rows_ref[place[0], at] = own_ref[at]
        rows_ref[place[1], at] = right_ref[at]
        rows_ref[place[7], at] = left_ref[at]
        rows_ref[place[3], at] = above_ref[at]
        rows_ref[place[5], at] = below_ref[at]
        rows_ref[place[2], at] = left_ref[pl.ds(count + start, block)]
        rows_ref[place[6], at] = right_ref[pl.ds(count + start, block)]
        if start < half:
            rows_ref[place[4], at] = left_ref[pl.ds(2 * count + start, block)]
        else:
            rows_ref[place[4], at] = right_ref[pl.ds(2 * count + start - half, block)]
        values = jnp.concatenate([rows_ref[k, at] for k in range(RING)], axis=1)
        values = values.astype(jnp.float32)
        inverse = lax.rsqrt(jnp.mean(values * values, axis=1, keepdims=True) + 1e-05)
        normed = (values * inverse * gain_ref[...]).astype(jnp.bfloat16)
        preact = jnp.dot(normed, w_in_ref[...], preferred_element_type=jnp.float32)
        hidden = jax.nn.gelu(preact, approximate=True).astype(jnp.bfloat16)
        sums = jnp.dot(hidden, w_out_ref[...], preferred_element_type=jnp.float32)
        sums = sums.astype(jnp.bfloat16)
        for k in range(RING):
            sums_ref[k, at] = sums[:, k * width : (k + 1) * width]
        to_right_ref[at] = sums_ref[place[1], at]
        to_right_ref[second] = sums_ref[place[6], at]
        to_left_ref[at] = sums_ref[place[7], at]
        to_left_ref[second] = sums_ref[place[2], at]
        if start < half:
            to_right_ref[pl.ds(2 * count + start, block)] = sums_ref[place[4], at]
        else:
            third = pl.ds(2 * count + start - half, block)
            to_left_ref[third] = sums_ref[place[4], at]
        keep_ref[0, at] = sums_ref[place[0], at]
        keep_ref[1, at] = sums_ref[place[3], at]
        keep_ref[2, at] = sums_ref[place[5], at]


def ffn_body(me_ref, *refs, block):
    branch(me_ref[0], *refs, block)


def pair_body(me_ref, *refs, block, later_block):
    own, below, above, left, right, gain, w_in, w_out = refs[:8]
    sources = refs[8:15]
    to_right, to_left, keep = refs[15:18]
    later_outs = refs[18:21]
    rows, sums, later_rows, later_sums = refs[21:25]
    targets = refs[25:32]
    done = refs[32]
    copies = [
        pltpu.make_async_copy(source, target, done.at[n])
        for n, (source, target) in enumerate(zip(sources, targets))
    ]
    for copy in copies:
        copy.start()
    me = me_ref[0]
    branch(
        me,
        own,
        below,
        above,
        left,
        right,
        gain,
        w_in,
        w_out,
        to_right,
        to_left,
        keep,
        rows,
        sums,
        block,
    )
    for copy in copies:
        copy.wait()
    branch(
        me,
        *targets[:5],
        gain,
        *targets[5:],
        *later_outs,
        later_rows,
        later_sums,
        later_block,
    )


def sums_of(count, width):
    return jax.ShapeDtypeStruct((3, count, width), jnp.bfloat16)


def tiles_of(count, width):
    return pltpu.VMEM((RING, count, width), jnp.bfloat16)


def estimate(count, model, hidden):
    return pl.CostEstimate(
        flops=4 * count * model * hidden,
        transcendentals=count * hidden,
        bytes_accessed=4 * count * model + 4 * model * hidden,
    )


def ffn(me, pieces, gain, w_in, w_out):
    count, width = pieces[0].shape
    model = RING * width
    vmem = pl.BlockSpec(memory_space=pltpu.VMEM)
    edge = jax.ShapeDtypeStruct((5 * count // 2, width), jnp.bfloat16)
    return pl.pallas_call(
        functools.partial(ffn_body, block=count // 4),
        in_specs=[pl.BlockSpec(memory_space=pltpu.SMEM)] + [vmem] * 8,
        out_specs=[vmem] * 3,
        out_shape=[edge, edge, sums_of(count, width)],
        scratch_shapes=[tiles_of(count, width)] * 2,
        compiler_params=pltpu.CompilerParams(vmem_limit_bytes=32 * 1024 * 1024),
        cost_estimate=estimate(count, model, w_in.shape[1]),
        name="exp",
    )(me, *pieces, gain.reshape(1, model), w_in, w_out)


def ffn_pair(me, pieces, gain, w_in, w_out, later_pieces, later_in, later_out):
    count, width = pieces[0].shape
    later = later_pieces[0].shape[0]
    model = RING * width
    vmem = pl.BlockSpec(memory_space=pltpu.VMEM)
    anywhere = pl.BlockSpec(memory_space=pl.ANY)
    edge = jax.ShapeDtypeStruct((5 * count // 2, width), jnp.bfloat16)
    later_edge = jax.ShapeDtypeStruct((5 * later // 2, width), jnp.bfloat16)
    operands = [*later_pieces, later_in, later_out]
    return pl.pallas_call(
        functools.partial(pair_body, block=count // 4, later_block=later // 4),
        in_specs=[pl.BlockSpec(memory_space=pltpu.SMEM)] + [vmem] * 8 + [anywhere] * 7,
        out_specs=[vmem] * 6,
        out_shape=[edge, edge, sums_of(count, width)]
        + [later_edge, later_edge, sums_of(later, width)],
        scratch_shapes=[tiles_of(count, width)] * 2
        + [tiles_of(later, width)] * 2
        + [pltpu.VMEM(value.shape, value.dtype) for value in operands]
        + [pltpu.SemaphoreType.DMA((7,))],
        compiler_params=pltpu.CompilerParams(vmem_limit_bytes=40 * 1024 * 1024),
        cost_estimate=estimate(count + later, model, w_in.shape[1]),
        name="pair",
    )(me, *pieces, gain.reshape(1, model), w_in, w_out, *operands)


def scatter_near(to_right, to_left):
    return shift(to_right, 1), shift(to_left, -1)


def scatter_far(keep, from_left, from_right):
    count = keep.shape[1]
    half = count // 2
    one, two = count, 2 * count

    def wide(value):
        return value.astype(jnp.float32)

    own = wide(keep[0]) + wide(from_left[:one]) + wide(from_right[:one])
    above = wide(keep[1]) + wide(from_right[one:two])
    to_above = jnp.concatenate(
        [above[:half] + wide(from_left[two : two + half]), above[half:]], axis=0
    )
    below = wide(keep[2]) + wide(from_left[one:two])
    to_below = jnp.concatenate(
        [below[:half], below[half:] + wide(from_right[two : two + half])], axis=0
    )
    first = shift(to_above.astype(jnp.bfloat16), 3)
    second = shift(to_below.astype(jnp.bfloat16), -3)
    return own, first, second


def per_device(
    tokens, gain, w_res_in, w_res_out, w_exp_in, w_exp_out, expert_of, slot_of, gate_prob
):
    row_count, feat_width = tokens.shape
    experts = lax.axis_size("expert")
    capacity = max(2, 5 * row_count // (4 * experts))
    slots = experts * capacity
    me = lax.axis_index("mp").astype(jnp.int32).reshape(1)
    slot_id = jnp.where(slot_of >= 0, expert_of * capacity + slot_of, -1)
    slot_index = jnp.arange(slots, dtype=jnp.int32)
    send_table = (slot_index[:, None] == slot_id[None, :]).astype(jnp.bfloat16)
    take_table = (slot_id[:, None] == slot_index[None, :]).astype(jnp.bfloat16)

    def exchange(rows):
        return lax.all_to_all(
            rows.reshape(experts, capacity, feat_width),
            "expert",
            split_axis=0,
            concat_axis=0,
            tiled=True,
        ).reshape(slots, feat_width)

    res_below = shift(tokens, 3)
    outgoing = jnp.dot(send_table, tokens, preferred_element_type=jnp.float32)
    outgoing = outgoing.astype(jnp.bfloat16)
    incoming = exchange(outgoing)
    res_above = shift(tokens, -3)
    res_left, res_right = gather_near(tokens, res_below, res_above)
    res_pieces = (tokens, res_below, res_above, res_left, res_right)
    chunk = slots // 2
    pieces = []
    for c in range(2):
        rows = incoming[c * chunk : (c + 1) * chunk]
        below, above = gather_far(rows)
        left, right = gather_near(rows, below, above)
        pieces.append((rows, below, above, left, right))
    to_right, to_left, keep_0 = ffn(me, pieces[0], gain, w_exp_in[0], w_exp_out[0])
    edges_0 = scatter_near(to_right, to_left)
    to_right, to_left, keep_1, res_to_right, res_to_left, res_keep = ffn_pair(
        me,
        pieces[1],
        gain,
        w_exp_in[0],
        w_exp_out[0],
        res_pieces,
        w_res_in,
        w_res_out,
    )
    edges_1 = scatter_near(to_right, to_left)
    res_edges = scatter_near(res_to_right, res_to_left)
    summed = []
    for keep, edges in ((keep_0, edges_0), (keep_1, edges_1)):
        own, first, second = scatter_far(keep, *edges)
        own = own + first.astype(jnp.float32) + second.astype(jnp.float32)
        summed.append(own.astype(jnp.bfloat16))

    returned = exchange(jnp.concatenate(summed, axis=0))
    res_own, res_first, res_second = scatter_far(res_keep, *res_edges)
    res_sum = res_own + res_first.astype(jnp.float32) + res_second.astype(jnp.float32)
    moe_value = jnp.dot(take_table, returned, preferred_element_type=jnp.float32)
    return (res_sum + gate_prob[:, None] * moe_value).astype(jnp.bfloat16)


def solution(mesh):
    return jax.shard_map(
        per_device,
        mesh=mesh,
        in_specs=(
            P(("groups", "expert"), "mp"),
            P(),
            P(None, "mp"),
            P("mp", None),
            P("expert", None, "mp"),
            P("expert", "mp", None),
            P(("groups", "expert")),
            P(("groups", "expert")),
            P(("groups", "expert")),
        ),
        out_specs=P(("groups", "expert"), "mp"),
        check_vma=False,
    )
```

```python
import functools

import jax
import jax.numpy as jnp
from jax import lax
from jax.experimental import pallas as pl
from jax.experimental.pallas import tpu as pltpu
from jax.sharding import PartitionSpec as P


RING = 8


def shift(value, step, axis="mp"):
    ring = lax.axis_size(axis)
    return lax.ppermute(value, axis, [(i, (i + step) % ring) for i in range(ring)])


def gather_far(own):
    below = shift(own, 3)
    above = shift(own, -3)
    return below, above


def gather_near(own, below, above):
    half = own.shape[0] // 2
    from_left = shift(jnp.concatenate([own, above, below[:half]], axis=0), 1)
    from_right = shift(jnp.concatenate([own, below, above[half:]], axis=0), -1)
    return from_left, from_right


def branch(
    me,
    own_ref,
    below_ref,
    above_ref,
    left_ref,
    right_ref,
    gain_ref,
    w_in_ref,
    w_out_ref,
    to_right_ref,
    to_left_ref,
    keep_ref,
    rows_ref,
    sums_ref,
    block,
):
    count, width = own_ref.shape
    half = count // 2
    place = [lax.rem(me + step, RING) for step in range(RING)]
    for start in range(0, count, block):
        at = pl.ds(start, block)
        second = pl.ds(count + start, block)
        rows_ref[place[0], at] = own_ref[at]
        rows_ref[place[1], at] = right_ref[at]
        rows_ref[place[7], at] = left_ref[at]
        rows_ref[place[3], at] = above_ref[at]
        rows_ref[place[5], at] = below_ref[at]
        rows_ref[place[2], at] = left_ref[pl.ds(count + start, block)]
        rows_ref[place[6], at] = right_ref[pl.ds(count + start, block)]
        if start < half:
            rows_ref[place[4], at] = left_ref[pl.ds(2 * count + start, block)]
        else:
            rows_ref[place[4], at] = right_ref[pl.ds(2 * count + start - half, block)]
        values = jnp.concatenate([rows_ref[k, at] for k in range(RING)], axis=1)
        values = values.astype(jnp.float32)
        inverse = lax.rsqrt(jnp.mean(values * values, axis=1, keepdims=True) + 1e-05)
        normed = (values * inverse * gain_ref[...]).astype(jnp.bfloat16)
        preact = jnp.dot(normed, w_in_ref[...], preferred_element_type=jnp.float32)
        hidden = jax.nn.gelu(preact, approximate=True).astype(jnp.bfloat16)
        sums = jnp.dot(hidden, w_out_ref[...], preferred_element_type=jnp.float32)
        sums = sums.astype(jnp.bfloat16)
        for k in range(RING):
            sums_ref[k, at] = sums[:, k * width : (k + 1) * width]
        to_right_ref[at] = sums_ref[place[1], at]
        to_right_ref[second] = sums_ref[place[6], at]
        to_left_ref[at] = sums_ref[place[7], at]
        to_left_ref[second] = sums_ref[place[2], at]
        if start < half:
            to_right_ref[pl.ds(2 * count + start, block)] = sums_ref[place[4], at]
        else:
            third = pl.ds(2 * count + start - half, block)
            to_left_ref[third] = sums_ref[place[4], at]
        keep_ref[0, at] = sums_ref[place[0], at]
        keep_ref[1, at] = sums_ref[place[3], at]
        keep_ref[2, at] = sums_ref[place[5], at]


def ffn_body(me_ref, *refs, block):
    branch(me_ref[0], *refs, block)


def pair_body(me_ref, *refs, block, later_block):
    own, below, above, left, right, gain, w_in, w_out = refs[:8]
    sources = refs[8:15]
    to_right, to_left, keep = refs[15:18]
    later_outs = refs[18:21]
    rows, sums, later_rows, later_sums = refs[21:25]
    targets = refs[25:32]
    done = refs[32]
    copies = [
        pltpu.make_async_copy(source, target, done.at[n])
        for n, (source, target) in enumerate(zip(sources, targets))
    ]
    for copy in copies:
        copy.start()
    me = me_ref[0]
    branch(
        me,
        own,
        below,
        above,
        left,
        right,
        gain,
        w_in,
        w_out,
        to_right,
        to_left,
        keep,
        rows,
        sums,
        block,
    )
    for copy in copies:
        copy.wait()
    branch(
        me,
        *targets[:5],
        gain,
        *targets[5:],
        *later_outs,
        later_rows,
        later_sums,
        later_block,
    )


def sums_of(count, width):
    return jax.ShapeDtypeStruct((3, count, width), jnp.bfloat16)


def tiles_of(count, width):
    return pltpu.VMEM((RING, count, width), jnp.bfloat16)


def estimate(count, model, hidden):
    return pl.CostEstimate(
        flops=4 * count * model * hidden,
        transcendentals=count * hidden,
        bytes_accessed=4 * count * model + 4 * model * hidden,
    )


def ffn(me, pieces, gain, w_in, w_out):
    count, width = pieces[0].shape
    model = RING * width
    vmem = pl.BlockSpec(memory_space=pltpu.VMEM)
    edge = jax.ShapeDtypeStruct((5 * count // 2, width), jnp.bfloat16)
    return pl.pallas_call(
        functools.partial(ffn_body, block=count // 2),
        in_specs=[pl.BlockSpec(memory_space=pltpu.SMEM)] + [vmem] * 8,
        out_specs=[vmem] * 3,
        out_shape=[edge, edge, sums_of(count, width)],
        scratch_shapes=[tiles_of(count, width)] * 2,
        compiler_params=pltpu.CompilerParams(vmem_limit_bytes=32 * 1024 * 1024),
        cost_estimate=estimate(count, model, w_in.shape[1]),
        name="exp",
    )(me, *pieces, gain.reshape(1, model), w_in, w_out)


def ffn_pair(me, pieces, gain, w_in, w_out, later_pieces, later_in, later_out):
    count, width = pieces[0].shape
    later = later_pieces[0].shape[0]
    model = RING * width
    vmem = pl.BlockSpec(memory_space=pltpu.VMEM)
    anywhere = pl.BlockSpec(memory_space=pl.ANY)
    edge = jax.ShapeDtypeStruct((5 * count // 2, width), jnp.bfloat16)
    later_edge = jax.ShapeDtypeStruct((5 * later // 2, width), jnp.bfloat16)
    operands = [*later_pieces, later_in, later_out]
    return pl.pallas_call(
        functools.partial(pair_body, block=count // 2, later_block=later // 2),
        in_specs=[pl.BlockSpec(memory_space=pltpu.SMEM)] + [vmem] * 8 + [anywhere] * 7,
        out_specs=[vmem] * 6,
        out_shape=[edge, edge, sums_of(count, width)]
        + [later_edge, later_edge, sums_of(later, width)],
        scratch_shapes=[tiles_of(count, width)] * 2
        + [tiles_of(later, width)] * 2
        + [pltpu.VMEM(value.shape, value.dtype) for value in operands]
        + [pltpu.SemaphoreType.DMA((7,))],
        compiler_params=pltpu.CompilerParams(vmem_limit_bytes=40 * 1024 * 1024),
        cost_estimate=estimate(count + later, model, w_in.shape[1]),
        name="pair",
    )(me, *pieces, gain.reshape(1, model), w_in, w_out, *operands)


def scatter_near(to_right, to_left):
    return shift(to_right, 1), shift(to_left, -1)


def scatter_far(keep, from_left, from_right):
    count = keep.shape[1]
    half = count // 2
    one, two = count, 2 * count

    def wide(value):
        return value.astype(jnp.float32)

    own = wide(keep[0]) + wide(from_left[:one]) + wide(from_right[:one])
    above = wide(keep[1]) + wide(from_right[one:two])
    to_above = jnp.concatenate(
        [above[:half] + wide(from_left[two : two + half]), above[half:]], axis=0
    )
    below = wide(keep[2]) + wide(from_left[one:two])
    to_below = jnp.concatenate(
        [below[:half], below[half:] + wide(from_right[two : two + half])], axis=0
    )
    first = shift(to_above.astype(jnp.bfloat16), 3)
    second = shift(to_below.astype(jnp.bfloat16), -3)
    return own, first, second


def per_device(
    tokens, gain, w_res_in, w_res_out, w_exp_in, w_exp_out, expert_of, slot_of, gate_prob
):
    row_count, feat_width = tokens.shape
    experts = lax.axis_size("expert")
    capacity = max(2, 5 * row_count // (4 * experts))
    slots = experts * capacity
    me = lax.axis_index("mp").astype(jnp.int32).reshape(1)
    slot_id = jnp.where(slot_of >= 0, expert_of * capacity + slot_of, -1)
    slot_index = jnp.arange(slots, dtype=jnp.int32)
    send_table = (slot_index[:, None] == slot_id[None, :]).astype(jnp.bfloat16)
    take_table = (slot_id[:, None] == slot_index[None, :]).astype(jnp.bfloat16)

    def exchange(rows):
        return lax.all_to_all(
            rows.reshape(experts, capacity, feat_width),
            "expert",
            split_axis=0,
            concat_axis=0,
            tiled=True,
        ).reshape(slots, feat_width)

    res_below = shift(tokens, 3)
    outgoing = jnp.dot(send_table, tokens, preferred_element_type=jnp.float32)
    outgoing = outgoing.astype(jnp.bfloat16)
    incoming = exchange(outgoing)
    res_above = shift(tokens, -3)
    res_left, res_right = gather_near(tokens, res_below, res_above)
    res_pieces = (tokens, res_below, res_above, res_left, res_right)
    chunk = slots // 2
    pieces = []
    for c in range(2):
        rows = incoming[c * chunk : (c + 1) * chunk]
        below, above = gather_far(rows)
        left, right = gather_near(rows, below, above)
        pieces.append((rows, below, above, left, right))
    to_right, to_left, keep_0 = ffn(me, pieces[0], gain, w_exp_in[0], w_exp_out[0])
    edges_0 = scatter_near(to_right, to_left)
    to_right, to_left, keep_1, res_to_right, res_to_left, res_keep = ffn_pair(
        me,
        pieces[1],
        gain,
        w_exp_in[0],
        w_exp_out[0],
        res_pieces,
        w_res_in,
        w_res_out,
    )
    edges_1 = scatter_near(to_right, to_left)
    res_edges = scatter_near(res_to_right, res_to_left)
    summed = []
    for keep, edges in ((keep_0, edges_0), (keep_1, edges_1)):
        own, first, second = scatter_far(keep, *edges)
        own = own + first.astype(jnp.float32) + second.astype(jnp.float32)
        summed.append(own.astype(jnp.bfloat16))

    returned = exchange(jnp.concatenate(summed, axis=0))
    res_own, res_first, res_second = scatter_far(res_keep, *res_edges)
    res_sum = res_own + res_first.astype(jnp.float32) + res_second.astype(jnp.float32)
    moe_value = jnp.dot(take_table, returned, preferred_element_type=jnp.float32)
    return (res_sum + gate_prob[:, None] * moe_value).astype(jnp.bfloat16)


def solution(mesh):
    return jax.shard_map(
        per_device,
        mesh=mesh,
        in_specs=(
            P(("groups", "expert"), "mp"),
            P(),
            P(None, "mp"),
            P("mp", None),
            P("expert", None, "mp"),
            P("expert", "mp", None),
            P(("groups", "expert")),
            P(("groups", "expert")),
            P(("groups", "expert")),
        ),
        out_specs=P(("groups", "expert"), "mp"),
        check_vma=False,
    )
```
